32 devices in a mesh: freq: 4 (over y, core), ga: 8 (over z, x).
Axes of the slice: x: 2, y: 2, z: 4, core: 2. Of those that a mesh axis runs over, the one named last changes fastest.
Arguments:
- screened: bfloat16 [24, 8192, 8192], P('freq', None, 'ga'), may hold values from -0.0625 to 0.0625
- elements: bfloat16 [512, 8192], P(None, 'ga'), may hold values from -6 to 6
- energies: float32 [512], replicated, may hold values from -3 to 3
- occupied: int32 [512], replicated, may hold values 0 or 1
- nodes: float32 [24], replicated, may hold values from 0.1 to 10
- quad_weights: float32 [24], replicated, may hold values from 0.05 to 1
- slot_freq: int32 [24], P('freq'), may hold values from 0 to 23, each once
Outputs:
- sigma: float32 [512, 512], P('ga')
The draws below stay inside these ranges and needn't reach their ends.
All inputs are finite; a program needn't handle non-finite values.
Results may differ from the reference program's by a relative error of at most 0.0042.
Values may be sent and summed in bfloat16 or wider, within the bound.
No kernel may reach another device: no remote copies, remote signals or barrier semaphores. Data moves between devices by JAX's collectives and lax.ppermute only.
A program may use at most 192 MiB of HBM per device.

```python
import math
import jax
import jax.numpy as jnp
from jax import lax

NB = 512
NG = 8192
F_DEV = 6
FREQS = 24
N_FREQ = 4


def with_ends(entries, stream_key, low, largest):
    place = [jax.random.randint(jax.random.fold_in(stream_key, axis), (), 0, length) for axis, length in enumerate(entries.shape)]
    longest = entries.shape.index(max(entries.shape))
    next_to = place[:longest] + [(place[longest] + 1) % entries.shape[longest]] + place[longest + 1:]
    return entries.at[tuple(place)].set(low).at[tuple(next_to)].set(largest)


def raised(values, own_key, source, target, parts, factor):
    owner, partner = [(jnp.arange(values.shape[axis_at]) // (values.shape[axis_at] // parts)).reshape([-1 if axis == axis_at else 1 for axis in range(values.ndim)]) for axis_at in (source, target)]
    chosen = jax.random.permutation(own_key, parts)[partner]
    strong = (owner == chosen) | (owner == (partner + parts // 2) % parts)
    return jnp.where(strong, factor * values, values)


def block_scale(stream_key, dims, pieces, low, largest):
    def one(dim, blocks):
        steps = jax.random.uniform(jax.random.fold_in(jax.random.fold_in(stream_key, 6), dim), (blocks,), jnp.float32, low / len(pieces), largest / len(pieces))
        return jnp.repeat(jnp.exp(steps), dims[dim] // blocks).reshape((-1,) + (1,) * (len(dims) - dim - 1))

    loudness = one(*pieces[0])
    for cut in pieces[1:]:
        loudness = loudness * one(*cut)
    return loudness


def centred(rng, extent, spread, bound, shards=(), dtype=jnp.bfloat16):
    entries = spread * jax.random.normal(rng, extent, jnp.float32)
    if shards:
        entries = entries * block_scale(rng, extent, shards, -0.22, 0.18)
    return jnp.clip(entries, -bound, bound).astype(dtype)


def bell_draw_with(own_key, shape, spread, most, shards, heavy, dtype=jnp.bfloat16):
    entries = spread * jax.random.normal(own_key, shape, jnp.float32)
    if shards:
        entries = entries * block_scale(own_key, shape, shards, -0.22, 0.18)
    return jnp.clip(raised(entries, jax.random.fold_in(own_key, 3), *heavy), -most, most).astype(dtype)


def setup_inputs(seed: int = 0) -> dict:
    seeds = jax.random.split(jax.random.key(seed), 8)
    screened = centred(seeds[0], (FREQS, NG, NG), NG ** -0.5, 0.0625, ((0, 4), (2, 8)))
    elements = bell_draw_with(seeds[1], (NB, NG), 1.0, 6.0, ((1, 8),), (1, 0, 8, 2.0))
    energies = jnp.clip(jax.random.uniform(seeds[2], (NB,), jnp.float32, -3.0, 3.0), -3.0, 3.0)
    occupied = with_ends((jax.random.randint(seeds[3], (NB,), 0, 2) < 1).astype(jnp.int32), jax.random.fold_in(seeds[3], 1), 0, 1)
    nodes = jnp.clip(jnp.exp(jax.random.uniform(seeds[4], (FREQS,), jnp.float32, math.log(0.1), math.log(10.0))), 0.1, 10.0)
    quad_weights = jnp.clip(jnp.exp(jax.random.uniform(seeds[5], (FREQS,), jnp.float32, math.log(0.05), math.log(1.0))), 0.05, 1.0)
    slot_freq = jax.random.permutation(seeds[6], FREQS).astype(jnp.int32)
    return dict(screened=screened, elements=elements, energies=energies, occupied=occupied, nodes=nodes, quad_weights=quad_weights, slot_freq=slot_freq)


SCISSOR = 0.5

def reference(screened, elements, energies, occupied, nodes, quad_weights, slot_freq):
    shift = energies + SCISSOR * (1.0 - 2.0 * occupied.astype(jnp.float32))
    node = nodes[slot_freq]
    weight = quad_weights[slot_freq]
    coeff = weight[:, None] * shift[None, :] / (shift[None, :] * shift[None, :] + node[:, None] * node[:, None])
    slabs = screened.reshape(N_FREQ, F_DEV, NG, NG)
    coeffs = coeff.reshape(N_FREQ, F_DEV, NB)

    def one_group(total, group):
        group_slabs, group_coeff = group

        def one_slab(acc, slab):
            matrix, factor = slab
            return (acc + factor[:, None] * jnp.dot(elements, matrix, preferred_element_type=jnp.float32), None)
        summed, unused = lax.scan(one_slab, jnp.zeros((NB, NG), jnp.float32), (group_slabs, group_coeff))
        weighted = summed.astype(jnp.bfloat16)
        term = lax.dot_general(weighted, elements, (((1,), (1,)), ((), ())), preferred_element_type=jnp.float32)
        return (total + term, None)
    total, unused = lax.scan(one_group, jnp.zeros((NB, NB), jnp.float32), (slabs, coeffs))
    return total / math.sqrt(NG)
```

```python
import functools
import math

import jax
import jax.numpy as jnp
from jax import lax
from jax.experimental import pallas as pl
from jax.experimental.pallas import tpu as pltpu
from jax.sharding import PartitionSpec as P

SCISSOR = 0.5
LANES = 128
VMEM = 26 << 20


def ring_at(place, count):
    return jnp.where(place < count // 2, 2 * place, 2 * (count - 1 - place) + 1)


def place_of(index, count):
    return jnp.where(index % 2 == 0, index // 2, count - 1 - index // 2)


def packed(rows, width):
    row = lax.broadcasted_iota(jnp.int32, (8, width), 0)
    table = jnp.zeros((8, width), jnp.float32)
    for i, r in enumerate(rows):
        line = jnp.pad(r.astype(jnp.float32), (0, width - r.shape[0]))
        table = jnp.where(row == i, line[None, :], table)
    return table


def coefficients(table, coeff):
    frequencies, bands, _ = coeff.shape
    row = table[0:1, :] + SCISSOR * (1.0 - 2.0 * table[1:2, :])
    shift = jnp.broadcast_to(row, (LANES, bands)).T
    square = shift * shift
    points = lax.broadcasted_iota(jnp.int32, (1, bands), 1).astype(jnp.float32)
    for j in range(frequencies):
        here = points == table[4:5, j : j + 1]
        node = jnp.sum(jnp.where(here, table[2:3, :], 0.0), axis=1, keepdims=True)
        weight = jnp.sum(jnp.where(here, table[3:4, :], 0.0), axis=1, keepdims=True)
        coeff[j] = weight * shift / (square + node * node)


def row_starts(piece, count, depth):
    kind, offset, part = piece
    core = lax.axis_index("freq") % 2
    place = place_of(lax.axis_index("ga"), count)
    way = 2 * core - 1
    half = depth // 2

    def shard(steps):
        return ring_at((place + way * steps + count) % count, count) * depth

    if kind == "pair":
        at = shard(offset) + part * half, shard(-offset) + part * half
    elif kind == "split":
        at = shard(offset) + core * half, shard(offset) + (1 - core) * half
    else:
        at = shard(offset), shard(offset) + half
    return tuple(pl.multiple_of(a, half) for a in at)


def project(pieces, after, first, last, count, n_freq, scale, *refs):
    refs = list(refs)
    take = lambda n: [refs.pop(0) for _ in range(n)]
    given = take(1)
    blocks = [take(2) for _ in pieces]
    (screened,) = take(1)
    ready, before = (None, None) if first else take(2)[::-1]
    own = take(1)[0] if last else None
    if last:
        keep, send = take(2)
        acc = take(1)[0]
    else:
        acc, handed = take(2)
    stored = take(1)[0] if first else given[0]
    coeff, settled, buffers, joined, arrived = take(5)

    slots, depth, width = buffers.shape
    unroll = slots // 2
    half = depth // 2
    frequencies = screened.shape[0]
    turns = frequencies // unroll
    starts = [row_starts(piece, count, depth) for piece in [*pieces, *after]]

    def fetch(at, j, slot):
        for side in range(2):
            pltpu.make_async_copy(
                screened.at[j, pl.ds(at[side], half), :],
                buffers.at[slot, pl.ds(side * half, half), :],
                arrived.at[slot],
            ).start()

    def await_slot(slot):
        pltpu.make_async_copy(
            screened.at[0, pl.ds(0, depth), :], buffers.at[slot], arrived.at[slot]
        ).wait()

    for u in range(0 if first else 1, unroll):
        fetch(starts[0], u, u)
    if first:
        coefficients(given[0], coeff)
        storing = pltpu.make_async_copy(coeff, stored, settled.at[0])
        storing.start()
        acc[...] = jnp.zeros_like(acc)
    else:
        loading = pltpu.make_async_copy(stored, coeff, settled.at[0])
        loading.start()
        buffers[0] = ready[...]
        if last:
            acc[...] = before[...]
        loading.wait()
    if after:
        passing = [
            pltpu.make_async_copy(
                screened.at[0, pl.ds(starts[-1][side], half), :],
                handed.at[pl.ds(side * half, half), :],
                settled.at[1 + side],
            )
            for side in range(2)
        ]

    for index in range(len(pieces)):
        joined[:, :half] = blocks[index][0][...]
        joined[:, half:] = blocks[index][1][...]

        def group(turn, carry, index=index):
            base = lax.rem(index * turns + turn, 2) * unroll
            beyond = unroll - base
            within = turn < turns - 1
            begin = jnp.where(within, (turn + 1) * unroll, 0)
            follows = index + 1 < len(pieces)
            nearby = starts[index]
            coming = starts[index + 1] if follows else nearby
            at = [
                pl.multiple_of(jnp.where(within, n, c), half) for n, c in zip(nearby, coming)
            ]

            @pl.when(within | follows)
            def _():
                for u in range(unroll):
                    fetch(at, begin + u, beyond + u)

            if after and not follows:

                @pl.when(turn == turns - 1)
                def _():
                    for copy in passing:
                        copy.start()

            for u in range(unroll):
                if index == 0 and not first and u == 0:

                    @pl.when(turn > 0)
                    def _():
                        await_slot(base + u)

                else:
                    await_slot(base + u)
                product = jnp.dot(
                    joined[...], buffers[base + u], preferred_element_type=jnp.float32
                )
                factor = coeff[turn * unroll + u]
                for lane in range(0, width, LANES):
                    acc[:, lane : lane + LANES] += factor * product[:, lane : lane + LANES]
            return carry

        lax.fori_loop(0, turns, group, 0)

    if after:
        for copy in passing:
            copy.wait()
    if first:
        storing.wait()

    if last:
        weighted = acc[...].astype(jnp.bfloat16)
        term = scale * lax.dot_general(
            weighted, own[...], (((1,), (1,)), ((), ())), preferred_element_type=jnp.float32
        )
        share = term.shape[0] // (count * n_freq)
        core = lax.axis_index("freq") % 2
        for choice in range(2):

            @pl.when(core == choice)
            def _():
                for g in range(count):
                    for q in range(n_freq):
                        to = keep if q % 2 == choice else send
                        at = (q // 2 * count + g) * share
                        by = (g * n_freq + q) * share
                        to[at : at + share, :] = term[by : by + share, :]


def call(pieces, arrays, given, screened, count, n_freq, after=(), state=None, own=None, scale=1.0):
    first, last = state is None, own is not None
    frequencies, total, width = screened.shape
    depth = total // count
    bands = arrays[0].shape[0]
    unroll = next(u for u in (3, 2, 1) if frequencies % (2 * u) == 0)
    vmem = pl.BlockSpec(memory_space=pltpu.VMEM)
    hbm = pl.BlockSpec(memory_space=pltpu.HBM)
    operands = [*given, *arrays, screened]
    specs = [vmem if first else hbm] + [vmem] * len(arrays) + [hbm]
    aliases = {}
    if not first:
        if not last:
            aliases = {len(operands): 0}
        operands += state
        specs += [vmem] * 2
    if last:
        operands.append(own)
        specs.append(vmem)
    sums = jax.ShapeDtypeStruct((bands, width), jnp.float32)
    factors = (frequencies, bands, LANES)
    scratch = []
    if last:
        outs = [jax.ShapeDtypeStruct((bands // 2, bands), jnp.float32)] * 2
        scratch.append(pltpu.VMEM(sums.shape, jnp.float32))
    else:
        outs = [sums, jax.ShapeDtypeStruct((depth, width), screened.dtype)]
    out_specs = [vmem] * 2
    if first:
        outs.append(jax.ShapeDtypeStruct(factors, jnp.float32))
        out_specs.append(hbm)
    scratch += [
        pltpu.VMEM(factors, jnp.float32),
        pltpu.SemaphoreType.DMA((3,)),
        pltpu.VMEM((2 * unroll, depth, width), screened.dtype),
        pltpu.VMEM((bands, depth), jnp.bfloat16),
        pltpu.SemaphoreType.DMA((2 * unroll,)),
    ]
    work = len(pieces) * frequencies * depth * width
    return pl.pallas_call(
        functools.partial(project, pieces, after, first, last, count, n_freq, scale),
        out_shape=outs,
        in_specs=specs,
        out_specs=out_specs,
        scratch_shapes=scratch,
        input_output_aliases=aliases,
        compiler_params=pltpu.CompilerParams(vmem_limit_bytes=VMEM),
        cost_estimate=pl.CostEstimate(
            flops=2 * bands * work, bytes_accessed=2 * work, transcendentals=0
        ),
    )(*operands)


def solution(mesh):
    count, n_freq = mesh.shape["ga"], mesh.shape["freq"]
    axes = ("freq", "ga")
    half = count // 2
    ring = [2 * p if p < half else 2 * (count - 1 - p) + 1 for p in range(count)]
    places = {g: p for p, g in enumerate(ring)}

    def permutation(move):
        pairs = []
        for f in range(n_freq):
            for g in range(count):
                to_f, to_g = move(f, g)
                pairs.append((f * count + g, to_f * count + to_g))
        return pairs

    onward = permutation(
        lambda f, g: (f, ring[(places[g] + (1 if f % 2 == 0 else -1)) % count])
    )
    partner = permutation(lambda f, g: (f ^ 1, g))

    def send(value, pairs):
        return lax.ppermute(value, axes, pairs)

    def body(screened, elements, energies, occupied, nodes, quad_weights, slot_freq):
        core = lax.axis_index("freq") % 2
        depth = elements.shape[1]
        table = packed(
            [energies, occupied, nodes, quad_weights, slot_freq], elements.shape[0]
        )
        here = [elements[:, : depth // 2], elements[:, depth // 2 :]]
        moved = [send(h, onward) for h in here]
        plan = [("cols", 0, 0), ("pair", 1, 0), ("pair", 1, 1)]
        for t in range(2, half):
            plan += [("cols", t, 0), ("cols", -t, 0)]
        plan.append(("split", half, 0))
        run = functools.partial(call, screened=screened, count=count, n_freq=n_freq)

        def step(arrays, given, **more):
            piece = plan.pop(0)
            return run([piece], arrays, [given], after=plan[:1], **more)

        acc, ready, coeff = step(here, table)

        onto = []
        for part in range(2):
            piece, acc = lax.optimization_barrier((moved[part], acc))
            onto.append(send(piece, onward))
            other = send(piece, partner)
            acc, ready = step([piece, other], coeff, state=[acc, ready])
        moved = onto
        for t in range(2, half):
            *here, acc = lax.optimization_barrier((*moved, acc))
            if t < half - 1:
                moved = [send(h, onward) for h in here]
            else:
                moved = [send(jnp.where(core == 0, *here), onward)]
            other = [send(h, partner) for h in here]
            acc, ready = step(here, coeff, state=[acc, ready])
            if t == half - 1:
                final, acc = lax.optimization_barrier((moved[0], acc))
                beside = send(final, partner)
            acc, ready = step(other, coeff, state=[acc, ready])
        keep, give = step(
            [final, beside],
            coeff,
            state=[acc, ready],
            own=elements,
            scale=1.0 / math.sqrt(depth * count),
        )
        return total(keep, give)

    def total(keep, give):
        f = lax.axis_index("freq")
        x = keep + send(give, partner)
        bit = 2
        while bit < n_freq:
            mine = f // bit % 2
            x = x.reshape(2, x.shape[0] // 2, x.shape[1])
            other = lax.dynamic_index_in_dim(x, 1 - mine, 0, keepdims=False)
            got = send(other.astype(jnp.bfloat16), permutation(lambda a, g: (a ^ bit, g)))
            x = lax.dynamic_index_in_dim(x, mine, 0, keepdims=False) + got.astype(jnp.float32)
            bit *= 2
        x = x.reshape(count, x.shape[0] // count, x.shape[1]).astype(jnp.bfloat16)
        x = jnp.sum(lax.all_to_all(x, "ga", 0, 0).astype(jnp.float32), axis=0)
        return lax.all_gather(x, "freq", axis=0, tiled=True)

    return jax.shard_map(
        body,
        mesh=mesh,
        in_specs=(P("freq", None, "ga"), P(None, "ga"), P(), P(), P(), P(), P("freq")),
        out_specs=P("ga", None),
        check_vma=False,
    )
```

```python
import functools
import math

import jax
import jax.numpy as jnp
from jax import lax
from jax.experimental import pallas as pl
from jax.experimental.pallas import tpu as pltpu
from jax.sharding import PartitionSpec as P

SCISSOR = 0.5
LANES = 128
VMEM = 26 << 20


def ring_at(place, count):
    return jnp.where(place < count // 2, 2 * place, 2 * (count - 1 - place) + 1)


def place_of(index, count):
    return jnp.where(index % 2 == 0, index // 2, count - 1 - index // 2)


def packed(rows, width):
    row = lax.broadcasted_iota(jnp.int32, (8, width), 0)
    table = jnp.zeros((8, width), jnp.float32)
    for i, r in enumerate(rows):
        line = jnp.pad(r.astype(jnp.float32), (0, width - r.shape[0]))
        table = jnp.where(row == i, line[None, :], table)
    return table


def coefficients(table, coeff):
    frequencies, bands, _ = coeff.shape
    row = table[0:1, :] + SCISSOR * (1.0 - 2.0 * table[1:2, :])
    shift = jnp.broadcast_to(row, (LANES, bands)).T
    square = shift * shift
    points = lax.broadcasted_iota(jnp.int32, (1, bands), 1).astype(jnp.float32)
    for j in range(frequencies):
        here = points == table[4:5, j : j + 1]
        node = jnp.sum(jnp.where(here, table[2:3, :], 0.0), axis=1, keepdims=True)
        weight = jnp.sum(jnp.where(here, table[3:4, :], 0.0), axis=1, keepdims=True)
        coeff[j] = weight * shift / (square + node * node)


def row_start(offset, count, depth):
    place = place_of(lax.axis_index("ga"), count)
    way = 2 * (lax.axis_index("freq") % 2) - 1
    at = ring_at((place + way * offset + count) % count, count) * depth
    return pl.multiple_of(at, depth)


def project(pieces, after, first, last, count, n_freq, scale, *refs):
    refs = list(refs)
    take = lambda n: [refs.pop(0) for _ in range(n)]
    given = take(1)
    blocks = take(len(pieces))
    (screened,) = take(1)
    ready, before = (None, None) if first else take(2)[::-1]
    own = take(1)[0] if last else None
    if last:
        keep, send = take(2)
        acc = take(1)[0]
    else:
        acc, handed = take(2)
    coeff = take(1)[0] if first else given[0]
    settled, buffers, arrived = take(3)

    slots, depth, width = buffers.shape
    unroll = slots // 2
    frequencies = screened.shape[0]
    turns = frequencies // unroll
    starts = [row_start(piece, count, depth) for piece in [*pieces, *after]]

    def fetch(at, j, slot):
        return pltpu.make_async_copy(
            screened.at[j, pl.ds(at, depth), :], buffers.at[slot], arrived.at[slot]
        )

    for u in range(0 if first else 1, unroll):
        fetch(starts[0], u, u).start()
    if first:
        coefficients(given[0], coeff)
        acc[...] = jnp.zeros_like(acc)
    else:
        buffers[0] = ready[...]
        if last:
            acc[...] = before[...]
    if after:
        passing = pltpu.make_async_copy(
            screened.at[0, pl.ds(starts[-1], depth), :], handed, settled
        )

    for index in range(len(pieces)):
        block = blocks[index]

        def group(turn, carry, index=index, block=block):
            base = lax.rem(index * turns + turn, 2) * unroll
            beyond = unroll - base
            within = turn < turns - 1
            begin = jnp.where(within, (turn + 1) * unroll, 0)
            follows = index + 1 < len(pieces)
            coming = starts[index + 1] if follows else starts[index]
            at = pl.multiple_of(jnp.where(within, starts[index], coming), depth)

            @pl.when(within | follows)
            def _():
                for u in range(unroll):
                    fetch(at, begin + u, beyond + u).start()

            if after and not follows:

                @pl.when(turn == turns - 1)
                def _():
                    passing.start()

            for u in range(unroll):
                if index == 0 and not first and u == 0:

                    @pl.when(turn > 0)
                    def _():
                        fetch(starts[index], 0, base + u).wait()

                else:
                    fetch(starts[index], 0, base + u).wait()
                product = jnp.dot(
                    block[...], buffers[base + u], preferred_element_type=jnp.float32
                )
                factor = coeff[turn * unroll + u]
                for lane in range(0, width, LANES):
                    acc[:, lane : lane + LANES] += factor * product[:, lane : lane + LANES]
            return carry

        lax.fori_loop(0, turns, group, 0)

    if after:
        passing.wait()

    if last:
        weighted = acc[...].astype(jnp.bfloat16)
        term = scale * lax.dot_general(
            weighted, own[...], (((1,), (1,)), ((), ())), preferred_element_type=jnp.float32
        )
        share = term.shape[0] // (count * 2)
        core = lax.axis_index("freq") % 2
        for choice in range(2):

            @pl.when(core == choice)
            def _():
                for g in range(count):
                    for q in range(2):
                        to = keep if q == choice else send
                        by = (g * 2 + q) * share
                        to[g * share : (g + 1) * share, :] = term[by : by + share, :]


def call(pieces, arrays, given, screened, count, n_freq, after=(), state=None, own=None, scale=1.0):
    first, last = state is None, own is not None
    frequencies, total, width = screened.shape
    depth = total // count
    bands = arrays[0].shape[0]
    unroll = next(u for u in (3, 2, 1) if frequencies % (2 * u) == 0)
    vmem = pl.BlockSpec(memory_space=pltpu.VMEM)
    hbm = pl.BlockSpec(memory_space=pltpu.HBM)
    operands = [*given, *arrays, screened]
    specs = [vmem] * (1 + len(arrays)) + [hbm]
    aliases = {}
    if not first:
        if not last:
            aliases = {len(operands): 0}
        operands += state
        specs += [vmem] * 2
    if last:
        operands.append(own)
        specs.append(vmem)
    sums = jax.ShapeDtypeStruct((bands, width), jnp.float32)
    factors = (frequencies, bands, LANES)
    scratch = []
    if last:
        outs = [jax.ShapeDtypeStruct((bands // 2, bands), jnp.float32)] * 2
        scratch.append(pltpu.VMEM(sums.shape, jnp.float32))
    else:
        outs = [sums, jax.ShapeDtypeStruct((depth, width), screened.dtype)]
    out_specs = [vmem] * 2
    if first:
        outs.append(jax.ShapeDtypeStruct(factors, jnp.float32))
        out_specs.append(vmem)
    scratch += [
        pltpu.SemaphoreType.DMA,
        pltpu.VMEM((2 * unroll, depth, width), screened.dtype),
        pltpu.SemaphoreType.DMA((2 * unroll,)),
    ]
    work = len(pieces) * frequencies * depth * width
    return pl.pallas_call(
        functools.partial(project, pieces, after, first, last, count, n_freq, scale),
        out_shape=outs,
        in_specs=specs,
        out_specs=out_specs,
        scratch_shapes=scratch,
        input_output_aliases=aliases,
        compiler_params=pltpu.CompilerParams(vmem_limit_bytes=VMEM),
        cost_estimate=pl.CostEstimate(
            flops=2 * bands * work, bytes_accessed=2 * work, transcendentals=0
        ),
    )(*operands)


def solution(mesh):
    count, n_freq = mesh.shape["ga"], mesh.shape["freq"]
    axes = ("freq", "ga")
    half = count // 2
    ring = [2 * p if p < half else 2 * (count - 1 - p) + 1 for p in range(count)]
    places = {g: p for p, g in enumerate(ring)}

    def permutation(move):
        pairs = []
        for f in range(n_freq):
            for g in range(count):
                to_f, to_g = move(f, g)
                pairs.append((f * count + g, to_f * count + to_g))
        return pairs

    onward = permutation(
        lambda f, g: (f, ring[(places[g] + (1 if f % 2 == 0 else -1)) % count])
    )
    partner = permutation(lambda f, g: (f ^ 1, g))

    def send(value, pairs):
        return lax.ppermute(value, axes, pairs)

    def body(screened, elements, energies, occupied, nodes, quad_weights, slot_freq):
        depth = elements.shape[1]
        table = packed(
            [energies, occupied, nodes, quad_weights, slot_freq], elements.shape[0]
        )
        moved = send(elements, onward)
        plan = [0]
        for t in range(1, half):
            plan += [t, -t]
        plan.append(half)
        run = functools.partial(call, screened=screened, count=count, n_freq=n_freq)

        def step(block, given, **more):
            piece = plan.pop(0)
            return run([piece], [block], [given], after=plan[:1], **more)

        acc, ready, coeff = step(elements, table)
        for t in range(1, half):
            here, acc = lax.optimization_barrier((moved, acc))
            moved = send(here, onward)
            other = send(here, partner)
            acc, ready = step(here, coeff, state=[acc, ready])
            acc, ready = step(other, coeff, state=[acc, ready])
        keep, give = step(
            moved,
            coeff,
            state=[acc, ready],
            own=elements,
            scale=1.0 / math.sqrt(depth * count),
        )
        return total(keep, give)

    def total(keep, give):
        x = keep + send(give, partner)
        x = x.reshape(count, x.shape[0] // count, x.shape[1]).astype(jnp.bfloat16)
        x = jnp.sum(lax.all_to_all(x, "ga", 0, 0).astype(jnp.float32), axis=0)
        bit = 2
        while bit < n_freq:
            x = x + send(x, permutation(lambda f, g: (f ^ bit, g)))
            bit *= 2
        other = send(x, partner)
        first = lax.axis_index("freq") % 2 == 0
        return jnp.concatenate([jnp.where(first, x, other), jnp.where(first, other, x)])

    return jax.shard_map(
        body,
        mesh=mesh,
        in_specs=(P("freq", None, "ga"), P(None, "ga"), P(), P(), P(), P(), P("freq")),
        out_specs=P("ga", None),
        check_vma=False,
    )
```
